32 devices in a mesh: mission: 2 (over x), arc: 16 (over z, y, core).
Axes of the slice: x: 2, y: 2, z: 4, core: 2. Of those that a mesh axis runs over, the one named last changes fastest.
Arguments:
- design: bfloat16 [2560, 5120], P(('mission', 'arc')), may hold values from -3 to 3
- nuisance_design: bfloat16 [2560, 128], P(('mission', 'arc')), may hold values from -1 to 1
- observed: float32 [2560], P(('mission', 'arc')), may hold values from -6 to 6
- arc_of_row: int32 [2560], P(('mission', 'arc')), may hold values from 0 to 1, as said below
- nuis_size: int32 [64], P(('mission', 'arc')), may hold values from 32 to 128
- weight_index: int32 [2560], P(('mission', 'arc')), may hold values from 0 to 7
- kind_weight: float32 [8], replicated, may hold values from 0.3 to 3
- mission_weight: float32 [2], P('mission'), may hold values from 0.3 to 3
Outputs:
- normal_fold: float32 [2560, 5120], P(('mission', 'arc'))
- right_side: float32 [5120], P(('mission', 'arc'))
- tail_diagonal: float32 [2560], P(('mission', 'arc'))
The draws below stay inside these ranges and needn't reach their ends.
Inputs may be any that keep to these rules, and one draw needn't show every extreme that they name: `arc_of_row`: in each row block of 80 rows the rows of arc 0 come first and those of arc 1 follow; each arc has at least 20 rows.
All inputs are finite; a program needn't handle non-finite values.
Results may differ from the reference program's by a relative error of at most 0.019.
Values may be sent and summed in bfloat16 or wider, within the bound.
No kernel may reach another device: no remote copies, remote signals or barrier semaphores. Data moves between devices by JAX's collectives and lax.ppermute only.
A program may use at most 192 MiB of HBM per device.

```python
import math
import jax
import jax.numpy as jnp
from jax import lax

P_SIZE = 5120
NUIS = 128
KINDS = 8
ARCS_DEV = 2
OBS_DEV = 80
HALF = 2560
OBS = 2560
ARCS = 64
N_MISSION = 2
N_ARC = 16


def draw_design(key, part):
    noise_key = jax.random.fold_in(jax.random.fold_in(key, 11), 0)
    freq_key = jax.random.fold_in(jax.random.fold_in(key, 11), 1)
    phase_key = jax.random.fold_in(jax.random.fold_in(key, 11), 2)
    perm_key = jax.random.fold_in(jax.random.fold_in(key, 11), 4)
    columns = jnp.arange(P_SIZE, dtype=jnp.float32)
    noise_part = jnp.clip(jax.random.normal(noise_key, (OBS, P_SIZE), jnp.float32), -6.0, 6.0)
    mode_count = 4
    frequency = jnp.exp(jax.random.uniform(freq_key, (OBS, mode_count), jnp.float32, math.log(0.001), 0.0))
    phases = jax.random.uniform(phase_key, (OBS, mode_count), jnp.float32, -math.pi, math.pi)
    smooth = jnp.zeros((OBS, P_SIZE), jnp.float32)
    for mode_id in range(mode_count):
        smooth = smooth + jnp.cos(frequency[:, mode_id:mode_id + 1] * columns[None, :] + phases[:, mode_id:mode_id + 1])
    values = noise_part + math.sqrt(2.0 / mode_count) * smooth
    blocks = OBS // OBS_DEV
    block_width = P_SIZE // blocks
    target = jax.random.permutation(perm_key, blocks)
    row_block = jnp.arange(OBS, dtype=jnp.int32) // OBS_DEV
    col_block = jnp.arange(P_SIZE, dtype=jnp.int32) // block_width
    spike_gain = jnp.where(target[row_block][:, None] == col_block[None, :], 6.0, 1.0)
    scaled = values * spike_gain / math.sqrt(OBS)
    return jnp.clip(scaled, -3.0, 3.0).astype(jnp.bfloat16)


def draw_arc_of_row(key, part):
    blocks = OBS // OBS_DEV
    split_at = jax.random.randint(jax.random.fold_in(key, 23), (blocks, 1), OBS_DEV // 4, 3 * OBS_DEV // 4 + 1)
    position = jnp.arange(OBS_DEV, dtype=jnp.int32)[None, :]
    return (position >= split_at).astype(jnp.int32).reshape(OBS)


def touch_ends(values, rng, least, top_value):
    shape = values.shape
    index_at = [jax.random.randint(jax.random.fold_in(rng, axis), (), 0, shape[axis]) for axis in range(len(shape))]
    values = values.at[tuple(index_at)].set(least)
    longest = shape.index(max(shape))
    index_at[longest] = (index_at[longest] + 1) % shape[longest]
    return values.at[tuple(index_at)].set(top_value)


def block_levels(key, extent, pieces, least, top_value):
    loudness = 1.0
    for axis_at, parts in pieces:
        steps = jax.random.uniform(jax.random.fold_in(jax.random.fold_in(key, 6), axis_at), (parts,), jnp.float32, least / len(pieces), top_value / len(pieces))
        loudness = loudness * jnp.repeat(jnp.exp(steps), extent[axis_at] // parts).reshape((-1,) + (1,) * (len(extent) - 1 - axis_at))
    return loudness


def normal_values(key, dims, deviation, reach, cuts=(), held_as=jnp.bfloat16):
    level = block_levels(key, dims, cuts, -0.22, 0.18) if cuts else 1.0
    array = jax.random.normal(key, dims, jnp.float32) * deviation * level
    return jnp.minimum(jnp.maximum(array, -reach), reach).astype(held_as)


def setup_inputs(seed: int = 0) -> dict:
    keys = jax.random.split(jax.random.key(seed), 9)
    return {
        "design": draw_design(jax.random.fold_in(keys[8], 71), 0),
        "nuisance_design": normal_values(keys[1], (OBS, NUIS), (OBS_DEV // 2) ** -0.5, 1.0, ((0, 32),)),
        "observed": normal_values(keys[2], (OBS,), 1.0, 6.0, ((0, 32),), jnp.float32),
        "arc_of_row": draw_arc_of_row(jax.random.fold_in(keys[8], 71), 0),
        "nuis_size": touch_ends(jax.random.randint(keys[4], (ARCS,), NUIS // 4, NUIS + 1), jax.random.fold_in(keys[4], 1), NUIS // 4, NUIS).astype(jnp.int32),
        "weight_index": touch_ends(jax.random.randint(keys[5], (OBS,), 0, KINDS), jax.random.fold_in(keys[5], 1), 0, KINDS - 1).astype(jnp.int32),
        "kind_weight": jnp.clip(jnp.exp(jax.random.uniform(keys[6], (KINDS,), jnp.float32, math.log(0.3), math.log(3.0))), 0.3, 3.0),
        "mission_weight": jnp.clip(jnp.exp(math.log(3.0) - 2.3025851 * jax.random.uniform(keys[7], (N_MISSION,), jnp.float32) ** block_levels(keys[7], (N_MISSION,), ((0, 2),), -0.2, 0.2)), 0.3, 3.0),
    }


def local_system(design, nuisance_design, observed, arc_of_row, nuis_size, weight_index, kind_weight):
    kind_ids = jnp.arange(kind_weight.shape[0], dtype=jnp.int32)
    row_weight = jnp.sum(jnp.where(weight_index[:, None] == kind_ids[None, :], kind_weight[None, :], 0.0), axis=1)
    nuis_ids = jnp.arange(nuisance_design.shape[1], dtype=jnp.int32)
    eye_block = jnp.eye(nuisance_design.shape[1], dtype=jnp.float32)
    blocks = []
    solved = []
    solved_obs = []
    for arc_id in range(ARCS_DEV):
        col_mask = (nuis_ids < nuis_size[arc_id]).astype(jnp.bfloat16)
        in_arc = (arc_of_row == arc_id).astype(jnp.float32)
        masked = nuisance_design * col_mask[None, :]
        weighted = (masked.astype(jnp.float32) * (row_weight * in_arc)[:, None]).astype(jnp.bfloat16)
        normal_ll = jnp.dot(weighted.T.astype(jnp.float32), masked.astype(jnp.float32), preferred_element_type=jnp.float32) + eye_block
        coupling = jnp.dot(weighted.T.astype(jnp.float32), design.astype(jnp.float32), preferred_element_type=jnp.float32)
        obs_part = jnp.dot(weighted.T.astype(jnp.float32), observed, precision=lax.Precision.HIGHEST)
        factor = jnp.linalg.cholesky(normal_ll)
        blocks.append(weighted)
        solved.append(jax.scipy.linalg.cho_solve((factor, True), coupling).astype(jnp.bfloat16))
        solved_obs.append(jax.scipy.linalg.cho_solve((factor, True), obs_part))
    stacked = jnp.concatenate(blocks, axis=1)
    solved_all = jnp.concatenate(solved, axis=0)
    obs_all = jnp.concatenate(solved_obs, axis=0)
    reduced = (row_weight[:, None] * design.astype(jnp.float32) - jnp.dot(stacked.astype(jnp.float32), solved_all.astype(jnp.float32), preferred_element_type=jnp.float32)).astype(jnp.bfloat16)
    reduced_obs = (row_weight * observed - jnp.dot(stacked.astype(jnp.float32), obs_all, precision=lax.Precision.HIGHEST)).astype(jnp.bfloat16)
    right_term = jnp.dot(reduced_obs.astype(jnp.float32), design.astype(jnp.float32), preferred_element_type=jnp.float32)
    half_width = design.shape[1] // 2
    tail_term = jnp.sum(design[:, half_width:].astype(jnp.float32) * reduced[:, half_width:].astype(jnp.float32), axis=0)
    return (reduced, right_term, tail_term)

def reference(design, nuisance_design, observed, arc_of_row, nuis_size, weight_index, kind_weight, mission_weight):
    devices = N_MISSION * N_ARC
    col_ids = jnp.arange(P_SIZE, dtype=jnp.int32)
    row_ids = jnp.arange(HALF, dtype=jnp.int32)
    keep_upper = col_ids[None, :] >= row_ids[:, None]

    def per_block(totals, block_id):
        fold_total, right_total, tail_total = totals
        row_start = (block_id * OBS_DEV).astype(jnp.int32)
        arc_start = (block_id * ARCS_DEV).astype(jnp.int32)
        block_design = lax.dynamic_slice_in_dim(design, row_start, OBS_DEV, 0)
        block_nuis = lax.dynamic_slice_in_dim(nuisance_design, row_start, OBS_DEV, 0)
        block_obs = lax.dynamic_slice_in_dim(observed, row_start, OBS_DEV, 0)
        block_arcs = lax.dynamic_slice_in_dim(arc_of_row, row_start, OBS_DEV, 0)
        block_kinds = lax.dynamic_slice_in_dim(weight_index, row_start, OBS_DEV, 0)
        block_sizes = lax.dynamic_slice_in_dim(nuis_size, arc_start, ARCS_DEV, 0)
        weight = mission_weight[block_id // N_ARC]
        reduced, right_term, tail_term = local_system(block_design, block_nuis, block_obs, block_arcs, block_sizes, block_kinds, kind_weight)
        term_full = weight * jnp.dot(block_design.T.astype(jnp.float32), reduced.astype(jnp.float32), preferred_element_type=jnp.float32)
        folded = jnp.where(keep_upper, term_full[:HALF], term_full[::-1, ::-1][:HALF])
        rounded = lax.optimization_barrier(folded.astype(jnp.bfloat16))
        fold_total = fold_total + rounded.astype(jnp.float32)
        return ((fold_total, right_total + weight * right_term, tail_total + weight * tail_term), None)
    initial = (jnp.zeros((HALF, P_SIZE), jnp.float32), jnp.zeros((P_SIZE,), jnp.float32), jnp.zeros((HALF,), jnp.float32))
    totals, unused_out = lax.scan(per_block, initial, jnp.arange(devices, dtype=jnp.int32))
    return (totals[0], totals[1], totals[2])
```

```python
import functools

import jax
import jax.numpy as jnp
import numpy as np
from jax import lax
from jax.experimental import pallas as pl
from jax.experimental.pallas import tpu as pltpu
from jax.sharding import PartitionSpec as P

AXES = ("mission", "arc")
F32 = jnp.float32
BF16 = jnp.bfloat16

CORES = 2
CHIPS = 4
GROUP = CORES * CHIPS


class Plan:
    def __init__(self, mission, arc, obs, width, arcs):
        self.mission, self.arc, self.obs, self.width, self.arcs = mission, arc, obs, width, arcs
        self.half = width // 2
        self.devices = mission * arc
        self.rows = self.half // self.devices
        self.dests = self.devices // GROUP
        self.bits = self.dests.bit_length() - 1
        self.window = GROUP * self.rows
        self.chunk = self.half // CHIPS
        self.mine = self.half // GROUP
        self.right_rows = -(-2 * self.rows // 128)
        self.tail_rows = -(-self.rows // 128)
        self.slot = 4 * (-(-(self.right_rows + self.tail_rows) // 4))
        self.small = self.devices * self.slot


def place():
    m = lax.axis_index("mission")
    a = lax.axis_index("arc")
    block = m * (lax.axis_size("arc") // GROUP) + a // GROUP
    g = a % GROUP
    return block, g, g // CORES, g % CORES


def pieces(plan, owner):
    for core in range(CORES):
        for w in range(plan.dests):
            yield w * plan.window + (owner * CORES + core) * plan.rows


def flip(x):
    rows, cols = x.shape
    lane = lax.broadcasted_iota(jnp.int32, (rows, 128), 1)
    tiles = [x[:, i : i + 128] for i in range(0, cols, 128)]
    out = [jnp.take_along_axis(t, 127 - lane, axis=1) for t in tiles[::-1]]
    return jnp.concatenate(out, axis=1)


def split_kernel(plan, d_ref, lo_ref, hi_ref):
    _, _, q, _ = place()
    d = d_ref[...].astype(F32)
    upper = d[:, : plan.half]
    lower = flip(d[:, plan.half :])
    for owner in range(CHIPS):
        at = [upper[:, s : s + plan.rows] for s in pieces(plan, owner)]
        at += [lower[:, s : s + plan.rows] for s in pieces(plan, owner)]
        chunk = jnp.concatenate(at, axis=1).astype(BF16)
        e = owner ^ q

        @pl.when(e < 2)
        def _():
            lo_ref[e] = chunk

        @pl.when(e >= 2)
        def _():
            hi_ref[e - 2] = chunk


def to_column(row, eye):
    return jnp.sum(jnp.where(eye, jnp.broadcast_to(row, eye.shape), jnp.zeros((), row.dtype)), axis=1, keepdims=True)


def inverse(a):
    n = a.shape[0]
    lane = lax.broadcasted_iota(jnp.int32, (1, n), 1)
    sub = lax.broadcasted_iota(jnp.int32, (n, 1), 0)
    for k in range(n):
        pivot = 1.0 / a[k : k + 1, k : k + 1]
        row = a[k : k + 1, :]
        col = a[:, k : k + 1]
        scaled = row * pivot
        new = a - col * scaled
        new = jnp.where(lane == k, col * pivot, new)
        new = jnp.where(sub == k, jnp.where(lane == k, -pivot, scaled), new)
        a = new
    return -a


def dot(a, b):
    return jnp.dot(a, b, preferred_element_type=F32)


def halves(x):
    hi = x.astype(BF16)
    return hi, (x - hi.astype(F32)).astype(BF16)


def system_kernel(plan, d_ref, nuis_ref, obs_ref, arc_ref, kind_ref, size_ref, kw_ref, mw_ref, out_ref):
    n = plan.obs
    sub = lax.broadcasted_iota(jnp.int32, (n, n), 0)
    lane = lax.broadcasted_iota(jnp.int32, (n, n), 1)
    eye = sub == lane
    arc = arc_ref[...]
    kind = kind_ref[...]
    inv_w = jnp.zeros((1, n), F32)
    for k in range(kw_ref.shape[0]):
        inv_w = jnp.where(kind == k, 1.0 / jnp.full((1, n), kw_ref[k], F32), inv_w)
    size = jnp.zeros((1, n), jnp.int32)
    for j in range(plan.arcs):
        size = jnp.where(arc == j, size_ref[j], size)
    arc_col = to_column(arc.astype(F32), eye)
    size_col = to_column(size.astype(F32), eye)
    nuis = nuis_ref[...].astype(F32)
    ids = lax.broadcasted_iota(jnp.int32, nuis.shape, 1).astype(F32)
    masked = jnp.where(ids < size_col, nuis, 0.0).astype(BF16)
    gram = lax.dot_general(masked, masked, (((1,), (1,)), ((), ())), preferred_element_type=F32)
    a = jnp.where(arc_col == arc.astype(F32), gram, 0.0)
    a = a + jnp.where(eye, jnp.broadcast_to(inv_w, (n, n)), 0.0)
    k = inverse(a) * mw_ref[0]
    obs = obs_ref[...]
    z = jnp.sum(k * to_column(obs, eye), axis=0, keepdims=True)
    out_ref[:n, :n] = k
    k_hi, k_lo = halves(k)
    z_hi, z_lo = halves(z)
    d = d_ref[...]
    right = dot(z_hi, d) + dot(z_lo, d)
    low = d[:, plan.half :]
    tail = jnp.sum(low.astype(F32) * (dot(k_hi, low) + dot(k_lo, low)), axis=0, keepdims=True)
    for g in range(GROUP):
        for j in range(plan.dests):
            dev = j * GROUP + g
            row = n + (g * plan.dests + j) * plan.slot
            for s in range(0, 2 * plan.rows, 128):
                wide = min(128, 2 * plan.rows - s)
                at = dev * 2 * plan.rows + s
                out_ref[row + s // 128 : row + s // 128 + 1, :wide] = right[:, at : at + wide]
            row += plan.right_rows
            for s in range(0, plan.rows, 128):
                wide = min(128, plan.rows - s)
                at = dev * plan.rows + s
                out_ref[row + s // 128 : row + s // 128 + 1, :wide] = tail[:, at : at + wide]


def factor_kernel(plan, base_ref, *refs):
    n = plan.obs
    packs, blocks = refs[:GROUP], refs[GROUP : 2 * GROUP]
    lhs_ref, small_ref = refs[2 * GROUP :]
    block, g, _, core = place()
    base = base_ref[...]
    source = core * plan.mine + (base[0:1] ^ block) * plan.rows + base[1:2]
    pick = (lax.broadcasted_iota(jnp.int32, (plan.chunk, plan.mine), 0) == source).astype(F32).astype(BF16)
    parts = []
    for pack, d_ref in zip(packs, blocks, strict=True):
        k_hi, k_lo = halves(pack[:n, :n])
        d = d_ref[0]
        both = [dot(d[:, s : s + plan.chunk], pick).astype(BF16) for s in (0, plan.chunk)]
        d = jnp.concatenate(both, axis=1)
        parts.append(dot(k_hi, d) + dot(k_lo, d))
    lhs_ref[...] = jnp.concatenate(parts, axis=0).T.astype(BF16)
    rows = plan.dests * plan.slot
    at = pl.multiple_of(n + g * rows, 8)
    total = packs[0][pl.ds(at, rows), :]
    for pack in packs[1:]:
        total = total + pack[pl.ds(at, rows), :]
    small_ref[...] = total


def fold_kernel(plan, step, row_ref, col_ref, lhs_ref, *refs):
    blocks, (keep_ref, send_ref) = refs[:GROUP], refs[GROUP:]
    block, g, q, _ = place()
    wide = plan.chunk
    rows = row_ref[...]
    row = (rows[:, 0:1] ^ block) * plan.window + g * plan.rows + rows[:, 1:2]
    col = col_ref[...] + (q ^ step) * (CORES * plan.rows)
    d = jnp.concatenate([b[0] for b in blocks], axis=0)
    lhs = lhs_ref[...]
    above, mirror = lhs[: plan.mine], lhs[plan.mine :]
    left = jnp.where(col >= row, dot(above, d[:, :wide]), dot(mirror, d[:, wide:])).astype(BF16)
    right = dot(above, d[:, wide:]).astype(BF16)
    count = plan.dests // 2
    for p in range(plan.dests):
        ref, at = (keep_ref, p) if p < count else (send_ref, p - count)
        span = slice(p * plan.rows, (p + 1) * plan.rows)
        ref[at, :, :wide] = left[span]
        ref[at, :, wide:] = right[span]


def finish_kernel(plan, terms, *refs):
    ins, (out_ref, right_ref, tail_ref, sum_ref) = refs[:-4], refs[-4:]
    small_refs, ins = ins[:2], ins[2:]
    block, _, q, _ = place()
    for step in range(CHIPS):
        total = ins[step * terms][0].astype(F32)
        for r in ins[step * terms + 1 : (step + 1) * terms]:
            total = total + r[0].astype(F32)
        sum_ref[step] = total
    upper = [None] * (plan.half // plan.rows)
    lower = [None] * (plan.half // plan.rows)
    for owner in range(CHIPS):
        chunk = sum_ref[owner ^ q]
        for i, s in enumerate(pieces(plan, owner)):
            upper[s // plan.rows] = chunk[:, i * plan.rows : (i + 1) * plan.rows]
            at = plan.chunk + i * plan.rows
            lower[s // plan.rows] = chunk[:, at : at + plan.rows]
    out_ref[:, : plan.half] = jnp.concatenate(upper, axis=1)
    out_ref[:, plan.half :] = flip(jnp.concatenate(lower, axis=1))
    small = small_refs[0][...] + small_refs[1][...]
    total = jnp.zeros((plan.slot, 128), F32)
    for j in range(plan.dests):
        total = jnp.where(block == j, small[j * plan.slot : (j + 1) * plan.slot], total)
    for s in range(0, 2 * plan.rows, 128):
        wide = min(128, 2 * plan.rows - s)
        right_ref[:, s : s + wide] = total[s // 128 : s // 128 + 1, :wide]
    for s in range(0, plan.rows, 128):
        wide = min(128, plan.rows - s)
        at = plan.right_rows + s // 128
        tail_ref[:, s : s + wide] = total[at : at + 1, :wide]


VMEM = pl.BlockSpec(memory_space=pltpu.VMEM)
SMEM = pl.BlockSpec(memory_space=pltpu.SMEM)


def shape(dims, dtype):
    return jax.ShapeDtypeStruct(dims, dtype)


def on_device(plan, design, nuis, observed, arc_of_row, nuis_size, weight_index, kind_weight, mission_weight):
    n, wide = plan.obs, 2 * plan.chunk

    def move(x, flip_bits):
        pairs = [(d, d ^ flip_bits) for d in range(plan.devices)]
        return lax.ppermute(x, AXES, pairs)

    half_shape = shape((CHIPS // 2, n, wide), BF16)
    low, high = pl.pallas_call(
        functools.partial(split_kernel, plan), out_shape=[half_shape, half_shape], in_specs=[VMEM], out_specs=[VMEM, VMEM], name="split"
    )(design)

    pack = pl.pallas_call(
        functools.partial(system_kernel, plan),
        out_shape=shape((n + plan.small, 128), F32),
        in_specs=[VMEM, VMEM, VMEM, VMEM, VMEM, SMEM, SMEM, SMEM],
        out_specs=VMEM,
        name="system",
    )(
        design,
        nuis,
        observed.reshape(1, n),
        arc_of_row.reshape(1, n),
        weight_index.reshape(1, n),
        nuis_size,
        kind_weight,
        mission_weight,
    )

    near, far = CORES, 2 * CORES
    near_a = move(low, near)
    far_a = move(high, far)
    across_a = move(far_a, near)
    across_b = move(near_a, far)
    near_b = move(high, near)
    far_b = move(low, far)
    first = [low, near_a, far_a, across_a]
    second = [high, near_b, far_b, across_b]
    slots = [0, 1, 0, 1]
    first += [move(x, 1) for x in first]
    second += [move(x, 1) for x in second]
    packs = [pack]
    packs.append(move(pack, near))
    packs.append(move(pack, far))
    packs.append(move(pack, near | far))
    packs += [move(x, 1) for x in packs]

    ids = np.arange(plan.mine)
    base = np.stack([ids // plan.rows, ids % plan.rows]).astype(np.int32)
    cols = np.concatenate([s + np.arange(plan.rows) for s in pieces(plan, 0)]).astype(np.int32)[None]

    def chunk_spec(slot):
        return pl.BlockSpec((1, n, wide), lambda i: (slot, 0, 0))

    def whole(dims):
        return pl.BlockSpec(dims, lambda i: (0,) * len(dims))

    lhs_shape = shape((2 * plan.mine, GROUP * n), BF16)
    small_shape = shape((plan.dests * plan.slot, 128), F32)
    lhs, small = pl.pallas_call(
        functools.partial(factor_kernel, plan),
        grid=(1,),
        out_shape=[lhs_shape, small_shape],
        in_specs=[whole(base.shape)]
        + [whole(pack.shape)] * GROUP
        + [chunk_spec(slots[b % CHIPS]) for b in range(GROUP)],
        out_specs=[whole(lhs_shape.shape), whole(small_shape.shape)],
        name="factor",
    )(jnp.asarray(base), *packs, *first)

    sizes = []
    count = plan.dests
    while count > 1:
        count //= 2
        sizes.append(count)

    def flat_bit(count):
        return count * GROUP

    keep_shape = shape((plan.dests // 2, plan.rows, wide), BF16)
    terms = []
    for step in range(CHIPS):
        blocks = first if step < 2 else second
        keep, sent = pl.pallas_call(
            functools.partial(fold_kernel, plan, step),
            grid=(1,),
            out_shape=[keep_shape, keep_shape],
            in_specs=[whole((plan.mine, 2)), whole(cols.shape), whole(lhs_shape.shape)]
            + [chunk_spec(slots[b % CHIPS] ^ (step % 2)) for b in range(GROUP)],
            out_specs=[whole(keep_shape.shape), whole(keep_shape.shape)],
            name=f"fold{step}",
        )(jnp.asarray(base.T), jnp.asarray(cols), lhs, *blocks)
        mine = [keep]
        for count in sizes:
            got = move(sent, flat_bit(count))
            mine.append(got)
            if count > 1:
                cut = count // 2
                sent = functools.reduce(jnp.add, [x[cut:count].astype(F32) for x in mine]).astype(BF16)
        terms.append(mine)

    for count in sizes[:-1]:
        small = small + move(small, flat_bit(count))
    other = move(small, flat_bit(sizes[-1]))

    flat = [x for mine in terms for x in mine]
    per = len(terms[0])
    fold, right, tail = pl.pallas_call(
        functools.partial(finish_kernel, plan, per),
        grid=(1,),
        out_shape=[
            shape((plan.rows, plan.width), F32),
            shape((1, 2 * plan.rows), F32),
            shape((1, plan.rows), F32),
        ],
        in_specs=[whole(small_shape.shape)] * 2 + [whole((1, plan.rows, wide))] * len(flat),
        out_specs=[whole((plan.rows, plan.width)), whole((1, 2 * plan.rows)), whole((1, plan.rows))],
        scratch_shapes=[pltpu.VMEM((CHIPS, plan.rows, wide), F32)],
        name="finish",
    )(small, other, *flat)
    return fold, right.reshape(2 * plan.rows), tail.reshape(plan.rows)


def solution(mesh):
    both = P(AXES)
    placed = (P(AXES, None), P(AXES, None), both, both, both, both, P(), P("mission"))

    def body(design, nuis, observed, arc_of_row, nuis_size, weight_index, kind_weight, mission_weight):
        plan = Plan(mesh.shape["mission"], mesh.shape["arc"], design.shape[0], design.shape[1], nuis_size.shape[0])
        return on_device(
            plan, design, nuis, observed, arc_of_row, nuis_size, weight_index, kind_weight, mission_weight
        )

    return jax.shard_map(
        body, mesh=mesh, in_specs=placed, out_specs=(P(AXES, None), both, both), check_vma=False
    )
```
